512 devices in a mesh: head: 8 (over y, core), seq: 64 (over z, x).
Axes of the slice: x: 4, y: 4, z: 16, core: 2. Of those that a mesh axis runs over, the one named last changes fastest.
Arguments:
- queries: bfloat16 [64, 1024, 4096], P('seq', 'head'), may hold values from -6 to 6
- key_rows: bfloat16 [64, 1024, 4096], P('seq', 'head'), may hold values from -6 to 6
- value_rows: bfloat16 [64, 1024, 4096], P('seq', 'head'), may hold values from -6 to 6
- head_gain: float32 [4096], replicated, may hold values from 0.5 to 1.5
Outputs:
- attended: bfloat16 [64, 1024, 4096], P('seq', 'head')
The draws below stay inside these ranges and needn't reach their ends.
All inputs are finite; a program needn't handle non-finite values.
Results may differ from the reference program's by a relative error of at most 0.0065.
Values may be sent and summed in bfloat16 or wider, within the bound.
No kernel may reach another device: no remote copies, remote signals or barrier semaphores. Data moves between devices by JAX's collectives and lax.ppermute only.
A program may use at most 64 MiB of HBM per device.

```python
import jax
import jax.numpy as jnp
from jax import lax

H = 32
DH = 128
BLOCK = 512
SPAN = 1024
N_SEQ = 64


def level_of(rng, dims, pieces, least, largest):
    def one(dim, parts):
        heights = jax.random.uniform(jax.random.fold_in(jax.random.fold_in(rng, 6), dim), (parts,), jnp.float32, least / len(pieces), largest / len(pieces))
        return jnp.repeat(jnp.exp(heights), dims[dim] // parts).reshape((-1,) + (1,) * (len(dims) - dim - 1))

    factor_of = one(*pieces[0])
    for cut in pieces[1:]:
        factor_of = factor_of * one(*cut)
    return factor_of


def normal_values(stream_key, dims, scale, reach, cuts=(), kind=jnp.bfloat16):
    values = jax.random.normal(stream_key, dims, jnp.float32) * scale
    if len(cuts) > 0:
        values = level_of(stream_key, dims, cuts, -0.22, 0.18) * values
    return jnp.clip(values, min=-reach, max=reach).astype(kind)


def setup_inputs(seed: int = 0) -> dict:
    streams_of = jax.random.split(jax.random.key(seed), 5)
    queries = normal_values(streams_of[0], (N_SEQ, SPAN, H * DH), 1.0, 6.0, ((0, 64), (1, 8)))
    key_rows = normal_values(streams_of[1], (N_SEQ, SPAN, H * DH), 1.0, 6.0, ((0, 64), (1, 8)))
    value_rows = normal_values(streams_of[2], (N_SEQ, SPAN, H * DH), 1.0, 6.0, ((0, 64), (1, 8)))
    head_gain = jnp.clip(1.0 + 0.1 * jax.random.normal(streams_of[3], (H * DH,), jnp.float32), 0.5, 1.5)
    return {"queries": queries, "key_rows": key_rows, "value_rows": value_rows, "head_gain": head_gain}


epsilon = 1e-06

def reference(queries, key_rows, value_rows, head_gain):
    seq_len = N_SEQ * SPAN
    blocks = seq_len // BLOCK
    q_all = queries.reshape(seq_len, H, DH)
    k_all = key_rows.reshape(seq_len, H, DH)
    v_all = value_rows.reshape(seq_len, H, DH)
    causal = jnp.tril(jnp.ones((BLOCK, BLOCK), dtype=bool))

    def one_head(head_index):
        head_q = lax.dynamic_index_in_dim(q_all, head_index, 1, keepdims=False)
        head_k = lax.dynamic_index_in_dim(k_all, head_index, 1, keepdims=False)
        head_v = lax.dynamic_index_in_dim(v_all, head_index, 1, keepdims=False)
        head_q = jax.nn.silu(head_q.astype(jnp.float32)).astype(jnp.bfloat16).reshape(blocks, BLOCK, DH)
        head_k = jax.nn.silu(head_k.astype(jnp.float32)).astype(jnp.bfloat16).reshape(blocks, BLOCK, DH)
        head_v = head_v.reshape(blocks, BLOCK, DH)

        def advance(carry_state, item):
            block_q, block_k, block_v = item
            scores = jnp.dot(block_q, block_k.T, preferred_element_type=jnp.float32)
            scores = jnp.where(causal, scores, 0.0).astype(jnp.bfloat16)
            local_part = jnp.dot(scores, block_v, preferred_element_type=jnp.float32)
            carried = jnp.dot(block_q.astype(jnp.float32), carry_state, precision=lax.Precision.HIGHEST)
            carry_state = carry_state + jnp.dot(block_k.T, block_v, preferred_element_type=jnp.float32)
            return (carry_state, local_part + carried)
        _, results = lax.scan(advance, jnp.zeros((DH, DH), jnp.float32), (head_q, head_k, head_v))
        results = results.reshape(seq_len, DH)
        normed = results * lax.rsqrt(lax.optimization_barrier(jnp.mean(results * results, axis=-1, keepdims=True)) + epsilon)
        return normed.astype(jnp.bfloat16)
    per_head = lax.map(one_head, jnp.arange(H, dtype=jnp.int32))
    normed = jnp.transpose(per_head, (1, 0, 2)).reshape(seq_len, H * DH)
    attended = (normed.astype(jnp.float32) * head_gain.astype(jnp.float32)).astype(jnp.bfloat16)
    return attended.reshape(N_SEQ, SPAN, H * DH)
```

```python
import jax
import jax.numpy as jnp
from jax import lax
from jax.experimental import pallas as pl
from jax.experimental.pallas import tpu as pltpu
from jax.sharding import Mesh
from jax.sharding import PartitionSpec as P

DH = 128
EPSILON = 1e-06
PLANE = ("x", "y", "core")
bf16 = jnp.bfloat16
f32 = jnp.float32


def silu(rows):
    x = rows.astype(f32)
    return (x * jax.nn.sigmoid(x)).astype(bf16)


def states_kernel(k_ref, v_ref, s_ref):
    for h in range(s_ref.shape[0]):
        cols = slice(h * DH, (h + 1) * DH)
        ka = silu(k_ref[0, :, cols])
        s_ref[h] = lax.dot_general(
            ka, v_ref[0, :, cols], (((0,), (0,)), ((), ())), preferred_element_type=f32
        ).astype(bf16)


def local_states(k, v, step):
    _, rows, width = k.shape
    heads = width // DH
    spec = pl.BlockSpec((1, rows, step * DH), lambda i: (0, 0, i))
    return pl.pallas_call(
        states_kernel,
        grid=(heads // step,),
        in_specs=[spec, spec],
        out_specs=pl.BlockSpec((step, DH, DH), lambda i: (i, 0, 0)),
        out_shape=jax.ShapeDtypeStruct((heads, DH, DH), bf16),
        name="states",
    )(k, v)


def total_kernel(s_ref, t_ref):
    total = s_ref[0].astype(f32)
    for r in range(1, s_ref.shape[0]):
        total = total + s_ref[r].astype(f32)
    t_ref[...] = total.astype(bf16)


def prefix_kernel(z_ref, s_ref, t_ref, p_ref):
    z = z_ref[0]
    running = jnp.zeros(t_ref.shape[1:], f32)
    for r in range(t_ref.shape[0]):
        running = running + jnp.where(r < z, t_ref[r].astype(f32), 0.0)
    for r in range(s_ref.shape[0]):
        p_ref[r] = running.astype(bf16)
        running = running + s_ref[r].astype(f32)


def output_kernel(q_ref, k_ref, v_ref, p_ref, g_ref, o_ref):
    rows = q_ref.shape[1]
    keep = lax.broadcasted_iota(jnp.int32, (rows, rows), 0) >= lax.broadcasted_iota(
        jnp.int32, (rows, rows), 1
    )
    for h in range(p_ref.shape[0]):
        cols = slice(h * DH, (h + 1) * DH)
        qa = silu(q_ref[0, :, cols])
        ka = silu(k_ref[0, :, cols])
        scores = lax.dot_general(qa, ka, (((1,), (1,)), ((), ())), preferred_element_type=f32)
        scores = jnp.where(keep, scores, 0.0).astype(bf16)
        o = jnp.dot(scores, v_ref[0, :, cols], preferred_element_type=f32)
        o = o + jnp.dot(qa, p_ref[h], preferred_element_type=f32)
        mean = jnp.mean(o * o, axis=-1, keepdims=True)
        normed = (o * lax.rsqrt(mean + EPSILON)).astype(bf16)
        o_ref[0, :, cols] = (normed.astype(f32) * g_ref[:, cols]).astype(bf16)


def outputs(q, k, v, prefix, gain, step):
    _, rows, width = q.shape
    heads = width // DH
    spec = pl.BlockSpec((1, rows, step * DH), lambda i: (0, 0, i))
    return pl.pallas_call(
        output_kernel,
        grid=(heads // step,),
        in_specs=[
            spec,
            spec,
            spec,
            pl.BlockSpec((step, DH, DH), lambda i: (i, 0, 0)),
            pl.BlockSpec((1, step * DH), lambda i: (0, i)),
        ],
        out_specs=spec,
        out_shape=jax.ShapeDtypeStruct(q.shape, bf16),
        name="outputs",
    )(q, k, v, prefix, gain)


def local(queries, key_rows, value_rows, head_gain):
    states = local_states(key_rows, value_rows, 8)
    mine = lax.all_to_all(states, PLANE, 0, 0, tiled=True)
    total = pl.pallas_call(
        total_kernel, out_shape=jax.ShapeDtypeStruct(mine.shape[1:], bf16), name="total"
    )(mine)
    totals = lax.all_gather(total, "z")
    z = lax.axis_index("z").astype(jnp.int32).reshape(1)
    vmem = pl.BlockSpec(memory_space=pltpu.VMEM)
    prefixes = pl.pallas_call(
        prefix_kernel,
        in_specs=[pl.BlockSpec(memory_space=pltpu.SMEM), vmem, vmem],
        out_specs=vmem,
        out_shape=jax.ShapeDtypeStruct(mine.shape, bf16),
        name="prefix",
    )(z, mine, totals)
    prefix = lax.all_to_all(prefixes, PLANE, 0, 0, tiled=True)
    return outputs(queries, key_rows, value_rows, prefix, head_gain[None, :], 8)


def solution(mesh):
    torus = Mesh(mesh.devices.reshape(4, 2, 16, 4), ("y", "core", "z", "x"))
    spec = P(("z", "x"), ("y", "core"), None)
    return jax.shard_map(
        local, mesh=torus, in_specs=(spec, spec, spec, P()), out_specs=spec, check_vma=False
    )
```

```python
import jax
import jax.numpy as jnp
from jax import lax
from jax.experimental import pallas as pl
from jax.experimental.pallas import tpu as pltpu
from jax.sharding import Mesh
from jax.sharding import PartitionSpec as P

DH = 128
STEP = 8
CHUNKS = 4
EPSILON = 1e-06
OWNERS = ("z2", "x", "y")
MIB = 2**20
bf16 = jnp.bfloat16
f32 = jnp.float32
VMEM = pl.BlockSpec(memory_space=pltpu.VMEM)
SMEM = pl.BlockSpec(memory_space=pltpu.SMEM)
HBM = pl.BlockSpec(memory_space=pltpu.HBM)


def params(mib):
    return pltpu.CompilerParams(vmem_limit_bytes=mib * MIB)


def stay(array):
    return pltpu.with_memory_space_constraint(array, pltpu.HBM)


def cost(flops):
    return pl.CostEstimate(flops=flops, bytes_accessed=2**21, transcendentals=0)


def silu(rows):
    x = rows.astype(f32)
    return (x * jax.nn.sigmoid(x)).astype(bf16)


def head_cols(h):
    return slice(h * DH, (h + 1) * DH)


def state(k, v):
    contract = (((0,), (0,)), ((), ()))
    return lax.dot_general(silu(k), v, contract, preferred_element_type=f32).astype(bf16)


def given_kernel(k_ref, v_ref, s_ref, k_buf, v_buf, k_sem, v_sem):
    half = 1 - lax.axis_index("core")
    width = k_buf.shape[2]
    heads = width // DH
    copies = []
    for c in range(CHUNKS):
        cols = pl.ds(pl.multiple_of((half * CHUNKS + c) * width, width), width)
        pair = (
            pltpu.make_async_copy(k_ref.at[0, :, cols], k_buf.at[c], k_sem.at[c]),
            pltpu.make_async_copy(v_ref.at[0, :, cols], v_buf.at[c], v_sem.at[c]),
        )
        for copy in pair:
            copy.start()
        copies.append(pair)
    for c in range(CHUNKS):
        for copy in copies[c]:
            copy.wait()
        for h in range(heads):
            s_ref[c * heads + h] = state(k_buf[c, :, head_cols(h)], v_buf[c, :, head_cols(h)])


def given_states(k, v):
    _, rows, width = k.shape
    heads = width // DH // 2
    chunk = (CHUNKS, rows, width // 2 // CHUNKS)
    return pl.pallas_call(
        given_kernel,
        in_specs=[HBM, HBM],
        out_specs=VMEM,
        out_shape=pltpu.VMEM((heads, DH, DH), bf16),
        scratch_shapes=[
            pltpu.VMEM(chunk, bf16),
            pltpu.VMEM(chunk, bf16),
            pltpu.SemaphoreType.DMA((CHUNKS,)),
            pltpu.SemaphoreType.DMA((CHUNKS,)),
        ],
        compiler_params=params(8),
        name="given",
    )(stay(k), stay(v))


def kept_kernel(half_ref, k_ref, v_ref, s_ref):
    for h in range(s_ref.shape[0]):
        s_ref[h] = state(k_ref[0, :, head_cols(h)], v_ref[0, :, head_cols(h)])


def kept_states(k, v, half):
    _, rows, width = k.shape
    heads = width // DH // 2
    spec = pl.BlockSpec((1, rows, width // 2), lambda i, half: (0, 0, half[0]))
    return pl.pallas_call(
        kept_kernel,
        grid_spec=pltpu.PrefetchScalarGridSpec(
            num_scalar_prefetch=1,
            grid=(1,),
            in_specs=[spec, spec],
            out_specs=pl.BlockSpec((heads, DH, DH), lambda i, half: (0, 0, 0)),
        ),
        out_shape=jax.ShapeDtypeStruct((heads, DH, DH), bf16),
        compiler_params=params(8),
        cost_estimate=cost(4 * 10**9),
        name="kept",
    )(half, k, v)


def within_kernel(half_ref, second_ref, q_ref, k_ref, v_ref, e_ref, qa_ref, o_ref):
    rows = q_ref.shape[1]
    keep = lax.broadcasted_iota(jnp.int32, (rows, rows), 0) >= lax.broadcasted_iota(
        jnp.int32, (rows, rows), 1
    )
    second = second_ref[0].astype(f32)
    for h in range(q_ref.shape[2] // DH):
        cols = head_cols(h)
        qa = silu(q_ref[0, :, cols])
        ka = silu(k_ref[0, :, cols])
        scores = lax.dot_general(qa, ka, (((1,), (1,)), ((), ())), preferred_element_type=f32)
        scores = jnp.where(keep, scores, 0.0).astype(bf16)
        qa_ref[0, :, cols] = qa
        here = jnp.dot(scores, v_ref[0, :, cols], preferred_element_type=f32)
        before = jnp.dot(qa, e_ref[h], preferred_element_type=f32)
        o_ref[0, :, cols] = here + second * before


def within(q, k, v, earlier, half, second):
    _, rows, width = q.shape
    blocks = width // DH // 2 // STEP
    tokens = (1, rows, STEP * DH)
    spec = pl.BlockSpec(tokens, lambda i, half, second: (0, 0, half[0] * blocks + i))
    out_spec = pl.BlockSpec(tokens, lambda i, half, second: (0, 0, i))
    shape = (1, rows, width // 2)
    return pl.pallas_call(
        within_kernel,
        grid_spec=pltpu.PrefetchScalarGridSpec(
            num_scalar_prefetch=2,
            grid=(blocks,),
            in_specs=[
                spec,
                spec,
                spec,
                pl.BlockSpec((STEP, DH, DH), lambda i, half, second: (i, 0, 0)),
            ],
            out_specs=[out_spec, out_spec],
        ),
        out_shape=[pltpu.HBM(shape, bf16), pltpu.HBM(shape, f32)],
        compiler_params=params(8),
        cost_estimate=cost(8 * 10**9),
        name="within",
    )(half, second, stay(q), stay(k), stay(v), earlier)


def total_kernel(s_ref, t_ref):
    total = s_ref[0].astype(f32)
    for r in range(1, s_ref.shape[0]):
        total = total + s_ref[r].astype(f32)
    total = total.astype(bf16)
    for r in range(t_ref.shape[0]):
        t_ref[r] = total


def prefix_kernel(z_ref, s_ref, t_ref, p_ref):
    z = z_ref[0]
    running = jnp.zeros(t_ref.shape[1:], f32)
    for r in range(t_ref.shape[0]):
        running = running + jnp.where(r < z, t_ref[r].astype(f32), 0.0)
    for r in range(s_ref.shape[0]):
        p_ref[r] = running.astype(bf16)
        running = running + s_ref[r].astype(f32)


def output_kernel(half_ref, qa_ref, o_ref, p_ref, g_ref, *rest):
    out_ref = rest[-1]
    for h in range(p_ref.shape[0]):
        cols = head_cols(h)
        o = o_ref[0, :, cols] + jnp.dot(qa_ref[0, :, cols], p_ref[h], preferred_element_type=f32)
        mean = jnp.mean(o * o, axis=-1, keepdims=True)
        normed = (o * lax.rsqrt(mean + EPSILON)).astype(bf16)
        out_ref[0, :, cols] = (normed.astype(f32) * g_ref[:, cols]).astype(bf16)


def half_outputs(qa, o, prefix, gain, half, before=None):
    _, rows, width = qa.shape
    tokens = pl.BlockSpec((1, rows, width), lambda i, half: (0, 0, 0))
    in_specs = [
        tokens,
        tokens,
        pl.BlockSpec(prefix.shape, lambda i, half: (0, 0, 0)),
        pl.BlockSpec((1, width), lambda i, half: (0, half[0])),
    ]
    operands = [qa, o, prefix, gain]
    if before is not None:
        in_specs.append(pl.BlockSpec(memory_space=pl.ANY))
        operands.append(before)
    return pl.pallas_call(
        output_kernel,
        grid_spec=pltpu.PrefetchScalarGridSpec(
            num_scalar_prefetch=1,
            grid=(1,),
            in_specs=in_specs,
            out_specs=pl.BlockSpec((1, rows, width), lambda i, half: (0, 0, half[0])),
        ),
        out_shape=jax.ShapeDtypeStruct((1, rows, 2 * width), bf16),
        input_output_aliases={} if before is None else {5: 0},
        compiler_params=params(8),
        cost_estimate=cost(4 * 10**9),
        name="outputs",
    )(half, *operands)


def attend(queries, key_rows, value_rows, head_gain):
    core = lax.axis_index("core").astype(jnp.int32)
    own, other = core.reshape(1), (1 - core).reshape(1)
    z = lax.axis_index("z8").astype(jnp.int32).reshape(1)
    gain = head_gain[None, :]
    own, other, z, gain = lax.optimization_barrier((own, other, z, gain))
    swap = ((0, 1), (1, 0))

    given = given_states(key_rows, value_rows)
    partner = lax.ppermute(given, "core", swap)
    kept = kept_states(key_rows, value_rows, own)
    chip = (kept.astype(f32) + partner.astype(f32)).astype(bf16)
    owners = lax.axis_size(OWNERS)
    pieces = (owners, chip.size // (owners * DH), DH)
    mine = lax.all_to_all(chip.reshape(pieces), OWNERS, 0, 0, tiled=True)
    kept, mine = lax.optimization_barrier((kept, mine))
    gift = lax.ppermute(kept, "core", ((0, 1),))
    planes = lax.axis_size("z8")
    total = pl.pallas_call(
        total_kernel,
        in_specs=[VMEM],
        out_specs=VMEM,
        out_shape=jax.ShapeDtypeStruct((planes,) + mine.shape[1:], bf16),
        compiler_params=params(8),
        name="total",
    )(mine)
    totals = lax.all_to_all(total, "z8", 0, 0, tiled=True)
    qa_own, o_own = within(queries, key_rows, value_rows, partner, own, own)
    qa_other, o_other = within(queries, key_rows, value_rows, gift, other, own)
    prefixes = pl.pallas_call(
        prefix_kernel,
        in_specs=[SMEM, VMEM, VMEM],
        out_specs=VMEM,
        out_shape=jax.ShapeDtypeStruct(mine.shape, bf16),
        compiler_params=params(8),
        name="prefix",
    )(z, mine, totals)
    before = lax.all_to_all(prefixes, OWNERS, 0, 0, tiled=True)
    before = before.reshape(chip.shape)
    arrived = lax.ppermute(before, "core", swap)
    out = half_outputs(qa_own, o_own, before, gain, own)
    return half_outputs(qa_other, o_other, arrived, gain, other, out)


def solution(mesh):
    torus = Mesh(mesh.devices.reshape(4, 2, 8, 2, 4), ("y", "core", "z8", "z2", "x"))
    spec = P(("z8", "z2", "x"), ("y", "core"), None)
    return jax.shard_map(
        attend, mesh=torus, in_specs=(spec, spec, spec, P()), out_specs=spec, check_vma=False
    )
```

```python
import functools

import jax
import jax.numpy as jnp
from jax import lax
from jax.experimental import pallas as pl
from jax.experimental.pallas import tpu as pltpu
from jax.sharding import Mesh
from jax.sharding import PartitionSpec as P


DH = 128
CHUNKS = 4
PARTS = 4
EARLY = 2
EPSILON = 1e-06
OWNERS = ("z2", "x", "y")
MIB = 2**20
bf16 = jnp.bfloat16
f32 = jnp.float32
VMEM = pl.BlockSpec(memory_space=pltpu.VMEM)
HBM = pl.BlockSpec(memory_space=pltpu.HBM)
DMA = pltpu.SemaphoreType.DMA


def params(mib):
    return pltpu.CompilerParams(vmem_limit_bytes=mib * MIB)


def stay(array):
    return pltpu.with_memory_space_constraint(array, pltpu.HBM)


def cost(flops):
    return pl.CostEstimate(flops=flops, bytes_accessed=2**21, transcendentals=0)


def silu(rows):
    x = rows.astype(f32)
    return (x * jax.nn.sigmoid(x)).astype(bf16)


def head_cols(h, start=0):
    return slice(start + h * DH, start + (h + 1) * DH)


def states_kernel(own, k_ref, v_ref, s_ref, k_buf, v_buf, sems):
    core = lax.axis_index("core")
    half = core if own else 1 - core
    width = k_buf.shape[1]
    cols = pl.ds(pl.multiple_of(half * width, width), width)
    copies = (
        pltpu.make_async_copy(k_ref.at[0, :, cols], k_buf, sems.at[0]),
        pltpu.make_async_copy(v_ref.at[0, :, cols], v_buf, sems.at[1]),
    )
    for copy in copies:
        copy.start()
    for copy in copies:
        copy.wait()
    for h in range(s_ref.shape[0]):
        s_ref[h] = lax.dot_general(
            silu(k_buf[:, head_cols(h)]),
            v_buf[:, head_cols(h)],
            (((0,), (0,)), ((), ())),
            preferred_element_type=f32,
        ).astype(bf16)


def half_states(k, v, own):
    _, rows, width = k.shape
    heads = width // DH // 2
    half = pltpu.VMEM((rows, width // 2), bf16)
    return pl.pallas_call(
        functools.partial(states_kernel, own),
        in_specs=[HBM, HBM],
        out_specs=VMEM,
        out_shape=pltpu.VMEM((heads, DH, DH), bf16),
        scratch_shapes=[half, half, DMA((2,))],
        compiler_params=params(8),
        cost_estimate=cost(4 * 10**9),
    )(stay(k), stay(v))


def within_kernel(low, high, *refs):
    z = lax.axis_index("z8")

    @pl.when(jnp.logical_and(z >= low, z < high))
    def _():
        within_body(*refs[:3], *refs[-9:])


def within_body(q_ref, k_ref, v_ref, own_ref, other_ref, q_buf, k_buf, buf, q_sem, k_sem, v_sem, out_sem):
    core = lax.axis_index("core")
    rows, width = q_buf.shape[1:]
    per_half = CHUNKS // 2
    keep = lax.broadcasted_iota(jnp.int32, (rows, rows), 0) >= lax.broadcasted_iota(
        jnp.int32, (rows, rows), 1
    )
    loads = []
    for c in range(CHUNKS):
        half = core if c < per_half else 1 - core
        block = half * per_half + c % per_half
        cols = pl.ds(pl.multiple_of(block * width, width), width)
        copies = (
            pltpu.make_async_copy(q_ref.at[0, :, cols], q_buf.at[c], q_sem.at[c]),
            pltpu.make_async_copy(k_ref.at[0, :, cols], k_buf.at[c], k_sem.at[c]),
            pltpu.make_async_copy(
                v_ref.at[0, :, cols], buf.at[c, :, pl.ds(2 * width, width)], v_sem.at[c]
            ),
        )
        for copy in copies:
            copy.start()
        loads.append(copies)
    stores = []
    for c in range(CHUNKS):
        for copy in loads[c]:
            copy.wait()
        for h in range(width // DH):
            qa = silu(q_buf[c, :, head_cols(h)])
            ka = silu(k_buf[c, :, head_cols(h)])
            scores = lax.dot_general(qa, ka, (((1,), (1,)), ((), ())), preferred_element_type=f32)
            buf[c, :, head_cols(2 * h)] = jnp.where(keep, scores, 0.0).astype(bf16)
            buf[c, :, head_cols(2 * h + 1)] = qa
        target = own_ref if c < per_half else other_ref
        cols = pl.ds((c % per_half) * 3 * width, 3 * width)
        store = pltpu.make_async_copy(buf.at[c], target.at[0, :, cols], out_sem.at[c])
        store.start()
        stores.append(store)
    for store in stores:
        store.wait()


def within(q, k, v, low, high, before):
    _, rows, width = q.shape
    chunk = width // CHUNKS
    out = pltpu.HBM((1, rows, 3 * width // 2), bf16)
    return pl.pallas_call(
        functools.partial(within_kernel, low, high),
        in_specs=[HBM] * 3 + [pl.BlockSpec(memory_space=pl.ANY)] * len(before),
        out_specs=[HBM, HBM],
        out_shape=[out, out],
        scratch_shapes=[
            pltpu.VMEM((CHUNKS, rows, chunk), bf16),
            pltpu.VMEM((CHUNKS, rows, chunk), bf16),
            pltpu.VMEM((CHUNKS, rows, 3 * chunk), bf16),
            DMA((CHUNKS,)),
            DMA((CHUNKS,)),
            DMA((CHUNKS,)),
            DMA((CHUNKS,)),
        ],
        input_output_aliases={3: 0, 4: 1} if low else {},
        compiler_params=params(12),
        cost_estimate=cost(8 * 10**9),
        name="within",
    )(stay(q), stay(k), stay(v), *before)


def merge_kernel(kept_ref, partner_ref, chip_ref, first_ref):
    early = lax.axis_index("core") == 0
    for h in range(kept_ref.shape[0]):
        kept, partner = kept_ref[h].astype(f32), partner_ref[h].astype(f32)
        chip_ref[h] = (kept + partner).astype(bf16)
        first_ref[h] = jnp.where(early, kept, partner).astype(bf16)


def total_kernel(s_ref, t_ref):
    total = s_ref[0].astype(f32)
    for r in range(1, s_ref.shape[0]):
        total = total + s_ref[r].astype(f32)
    t_ref[...] = total.astype(bf16)


def sum_kernel(*refs):
    total = refs[0][...].astype(f32)
    for t_ref in refs[1:-1]:
        total = total + t_ref[...].astype(f32)
    refs[-1][...] = total.astype(bf16)


def prefix_kernel(s_ref, *refs):
    p_ref = refs[-1]
    running = refs[0][...].astype(f32)
    for t_ref in refs[1:-1]:
        running = running + t_ref[...].astype(f32)
    for r in range(s_ref.shape[0]):
        p_ref[r] = running.astype(bf16)
        running = running + s_ref[r].astype(f32)


def hand_over_kernel(before_ref, first_ref, passed_ref, used_ref):
    early = lax.axis_index("core") == 0
    for h in range(before_ref.shape[0]):
        before, first = before_ref[h].astype(f32), first_ref[h].astype(f32)
        passed_ref[h] = (before + jnp.where(early, first, 0.0)).astype(bf16)
        used_ref[h] = (before + jnp.where(early, 0.0, first)).astype(bf16)


def on_chip(kernel, outs, *operands):
    shapes = [jax.ShapeDtypeStruct(shape, bf16) for shape in outs]
    return pl.pallas_call(
        kernel,
        in_specs=[VMEM] * len(operands),
        out_specs=[VMEM] * len(outs),
        out_shape=shapes,
        compiler_params=params(8),
    )(*operands)


def output_kernel(own, sqv_ref, p_ref, g_ref, *rest):
    out_ref, buf, sems = rest[-3:]
    core = lax.axis_index("core")
    half = core if own else 1 - core
    heads = p_ref.shape[0]
    parts, _, width = buf.shape
    per = 2 * heads // CHUNKS
    stores = []
    for h in range(heads):
        part, j = h // (heads // parts), h % (heads // parts)
        start = h // per * 3 * per * DH
        scores_qa = sqv_ref[0, :, start + 2 * (h % per) * DH : start + 2 * (h % per + 1) * DH]
        v = sqv_ref[0, :, head_cols(h % per, start + 2 * per * DH)]
        o = jnp.dot(
            scores_qa, jnp.concatenate([v, p_ref[h]], axis=0), preferred_element_type=f32
        )
        mean = jnp.mean(o * o, axis=-1, keepdims=True)
        normed = (o * lax.rsqrt(mean + EPSILON)).astype(bf16)
        gain = g_ref[:, pl.ds(pl.multiple_of(half * heads * DH + h * DH, DH), DH)]
        buf[part, :, head_cols(j)] = (normed.astype(f32) * gain).astype(bf16)
        if (h + 1) * DH == (part + 1) * width:
            cols = pl.ds(pl.multiple_of((half * parts + part) * width, width), width)
            store = pltpu.make_async_copy(buf.at[part], out_ref.at[0, :, cols], sems.at[part])
            store.start()
            stores.append(store)
    for store in stores:
        store.wait()


def half_outputs(sqv, prefix, gain, own, before=None):
    _, rows, width = sqv.shape
    width = width // 3
    in_specs, operands = [VMEM, VMEM, VMEM], [sqv, prefix, gain]
    if before is not None:
        in_specs.append(HBM)
        operands.append(before)
    return pl.pallas_call(
        functools.partial(output_kernel, own),
        in_specs=in_specs,
        out_specs=HBM,
        out_shape=jax.ShapeDtypeStruct((1, rows, 2 * width), bf16),
        scratch_shapes=[pltpu.VMEM((PARTS, rows, width // PARTS), bf16), DMA((PARTS,))],
        input_output_aliases={} if before is None else {3: 0},
        compiler_params=params(8),
        cost_estimate=cost(4 * 10**9),
        name="outputs",
    )(*operands)


def attend(queries, key_rows, value_rows, head_gain):
    swap = ((0, 1), (1, 0))
    owners, planes = lax.axis_size(OWNERS), lax.axis_size("z8")

    given = half_states(key_rows, value_rows, False)
    partner = lax.ppermute(given, "core", swap)
    kept = half_states(key_rows, value_rows, True)
    half = kept.shape
    chip, first = on_chip(merge_kernel, [half, half], kept, partner)
    pieces = (owners, chip.size // (owners * DH), DH)
    mine = lax.all_to_all(chip.reshape(pieces), OWNERS, 0, 0, tiled=True)
    (total,) = on_chip(total_kernel, [mine.shape[1:]], mine)
    span = planes // 2
    parts = within(queries, key_rows, value_rows, 0, EARLY, [total])
    total, *parts = lax.optimization_barrier((total, *parts))

    def ahead(k, value, low, high):
        return lax.ppermute(value, "z8", [(i, i + k) for i in range(low, high - k)])

    earlier = [ahead(k, total, 0, span - 1) for k in range(span - 2, 0, -1)]
    parts = within(queries, key_rows, value_rows, EARLY, span, parts)
    (front,) = on_chip(sum_kernel, [total.shape], total, *earlier)
    earlier.append(ahead(1, front, span - 2, span))
    (front,) = on_chip(sum_kernel, [total.shape], total, *earlier)
    earlier += [ahead(k, front, span - 1, planes) for k in range(planes - span, 0, -1)]
    sqv_own, sqv_other = within(queries, key_rows, value_rows, span, planes, parts)
    (prefixes,) = on_chip(prefix_kernel, [mine.shape], mine, *earlier)
    before = lax.all_to_all(prefixes, OWNERS, 0, 0, tiled=True)
    before = before.reshape(half)
    passed, used = on_chip(hand_over_kernel, [half, half], before, first)
    arrived = lax.ppermute(passed, "core", swap)
    gain = head_gain[None, :]
    out = half_outputs(sqv_own, used, gain, True)
    return half_outputs(sqv_other, arrived, gain, False, out)


def solution(mesh):
    torus = Mesh(mesh.devices.reshape(4, 2, 8, 2, 4), ("y", "core", "z8", "z2", "x"))
    spec = P(("z8", "z2", "x"), ("y", "core"), None)
    return jax.shard_map(
        attend, mesh=torus, in_specs=(spec, spec, spec, P()), out_specs=spec, check_vma=False
    )
```

```python
import functools

import jax
import jax.numpy as jnp
from jax import lax
from jax.experimental import pallas as pl
from jax.experimental.pallas import tpu as pltpu
from jax.sharding import Mesh
from jax.sharding import PartitionSpec as P


DH = 128
CHUNKS = 4
PARTS = 4
EARLY = 1
EPSILON = 1e-06
OWNERS = ("z2", "x", "y")
MIB = 2**20
bf16 = jnp.bfloat16
f32 = jnp.float32
VMEM = pl.BlockSpec(memory_space=pltpu.VMEM)
HBM = pl.BlockSpec(memory_space=pltpu.HBM)
DMA = pltpu.SemaphoreType.DMA


def params(mib):
    return pltpu.CompilerParams(vmem_limit_bytes=mib * MIB)


def stay(array):
    return pltpu.with_memory_space_constraint(array, pltpu.HBM)


def cost(flops):
    return pl.CostEstimate(flops=flops, bytes_accessed=2**21, transcendentals=0)


def silu(rows):
    x = rows.astype(f32)
    return (x * jax.nn.sigmoid(x)).astype(bf16)


def head_cols(h, start=0):
    return slice(start + h * DH, start + (h + 1) * DH)


def states_kernel(own, k_ref, v_ref, s_ref, k_buf, v_buf, sems):
    core = lax.axis_index("core")
    half = core if own else 1 - core
    width = k_buf.shape[1]
    cols = pl.ds(pl.multiple_of(half * width, width), width)
    copies = (
        pltpu.make_async_copy(k_ref.at[0, :, cols], k_buf, sems.at[0]),
        pltpu.make_async_copy(v_ref.at[0, :, cols], v_buf, sems.at[1]),
    )
    for copy in copies:
        copy.start()
    for copy in copies:
        copy.wait()
    for h in range(s_ref.shape[0]):
        s_ref[h] = lax.dot_general(
            silu(k_buf[:, head_cols(h)]),
            v_buf[:, head_cols(h)],
            (((0,), (0,)), ((), ())),
            preferred_element_type=f32,
        ).astype(bf16)


def half_states(k, v, own):
    _, rows, width = k.shape
    heads = width // DH // 2
    half = pltpu.VMEM((rows, width // 2), bf16)
    return pl.pallas_call(
        functools.partial(states_kernel, own),
        in_specs=[HBM, HBM],
        out_specs=VMEM,
        out_shape=pltpu.VMEM((heads, DH, DH), bf16),
        scratch_shapes=[half, half, DMA((2,))],
        compiler_params=params(8),
        cost_estimate=cost(4 * 10**9),
    )(stay(k), stay(v))


def within_kernel(low, high, *refs):
    z = lax.axis_index("z8")

    @pl.when(jnp.logical_and(z >= low, z < high))
    def _():
        within_body(*refs[:3], *refs[-9:])


def within_body(q_ref, k_ref, v_ref, own_ref, other_ref, q_buf, k_buf, buf, q_sem, k_sem, v_sem, out_sem):
    core = lax.axis_index("core")
    rows, width = q_buf.shape[1:]
    per_half = CHUNKS // 2
    keep = lax.broadcasted_iota(jnp.int32, (rows, rows), 0) >= lax.broadcasted_iota(
        jnp.int32, (rows, rows), 1
    )
    loads = []
    for c in range(CHUNKS):
        half = core if c < per_half else 1 - core
        block = half * per_half + c % per_half
        cols = pl.ds(pl.multiple_of(block * width, width), width)
        copies = (
            pltpu.make_async_copy(q_ref.at[0, :, cols], q_buf.at[c], q_sem.at[c]),
            pltpu.make_async_copy(k_ref.at[0, :, cols], k_buf.at[c], k_sem.at[c]),
            pltpu.make_async_copy(
                v_ref.at[0, :, cols], buf.at[c, :, pl.ds(2 * width, width)], v_sem.at[c]
            ),
        )
        for copy in copies:
            copy.start()
        loads.append(copies)
    stores = []
    for c in range(CHUNKS):
        for copy in loads[c]:
            copy.wait()
        for h in range(width // DH):
            qa = silu(q_buf[c, :, head_cols(h)])
            ka = silu(k_buf[c, :, head_cols(h)])
            scores = lax.dot_general(qa, ka, (((1,), (1,)), ((), ())), preferred_element_type=f32)
            buf[c, :, head_cols(2 * h)] = jnp.where(keep, scores, 0.0).astype(bf16)
            buf[c, :, head_cols(2 * h + 1)] = qa
        target = own_ref if c < per_half else other_ref
        cols = pl.ds((c % per_half) * 3 * width, 3 * width)
        store = pltpu.make_async_copy(buf.at[c], target.at[0, :, cols], out_sem.at[c])
        store.start()
        stores.append(store)
    for store in stores:
        store.wait()


def within(q, k, v, low, high, before):
    _, rows, width = q.shape
    chunk = width // CHUNKS
    out = pltpu.HBM((1, rows, 3 * width // 2), bf16)
    return pl.pallas_call(
        functools.partial(within_kernel, low, high),
        in_specs=[HBM] * 3 + [pl.BlockSpec(memory_space=pl.ANY)] * len(before),
        out_specs=[HBM, HBM],
        out_shape=[out, out],
        scratch_shapes=[
            pltpu.VMEM((CHUNKS, rows, chunk), bf16),
            pltpu.VMEM((CHUNKS, rows, chunk), bf16),
            pltpu.VMEM((CHUNKS, rows, 3 * chunk), bf16),
            DMA((CHUNKS,)),
            DMA((CHUNKS,)),
            DMA((CHUNKS,)),
            DMA((CHUNKS,)),
        ],
        input_output_aliases={3: 0, 4: 1} if low else {},
        compiler_params=params(12),
        cost_estimate=cost(8 * 10**9),
        name="within",
    )(stay(q), stay(k), stay(v), *before)


def merge_kernel(kept_ref, partner_ref, chip_ref, first_ref):
    early = lax.axis_index("core") == 0
    for h in range(kept_ref.shape[0]):
        kept, partner = kept_ref[h].astype(f32), partner_ref[h].astype(f32)
        chip_ref[h] = (kept + partner).astype(bf16)
        first_ref[h] = jnp.where(early, kept, partner).astype(bf16)


def total_kernel(s_ref, t_ref):
    total = s_ref[0].astype(f32)
    for r in range(1, s_ref.shape[0]):
        total = total + s_ref[r].astype(f32)
    t_ref[...] = total.astype(bf16)


def sum_kernel(*refs):
    total = refs[0][...].astype(f32)
    for t_ref in refs[1:-1]:
        total = total + t_ref[...].astype(f32)
    refs[-1][...] = total.astype(bf16)


def prefix_kernel(s_ref, *refs):
    p_ref = refs[-1]
    running = refs[0][...].astype(f32)
    for t_ref in refs[1:-1]:
        running = running + t_ref[...].astype(f32)
    for r in range(s_ref.shape[0]):
        p_ref[r] = running.astype(bf16)
        running = running + s_ref[r].astype(f32)


def hand_over_kernel(before_ref, first_ref, passed_ref, used_ref):
    early = lax.axis_index("core") == 0
    for h in range(before_ref.shape[0]):
        before, first = before_ref[h].astype(f32), first_ref[h].astype(f32)
        passed_ref[h] = (before + jnp.where(early, first, 0.0)).astype(bf16)
        used_ref[h] = (before + jnp.where(early, 0.0, first)).astype(bf16)


def on_chip(kernel, outs, *operands):
    shapes = [jax.ShapeDtypeStruct(shape, bf16) for shape in outs]
    return pl.pallas_call(
        kernel,
        in_specs=[VMEM] * len(operands),
        out_specs=[VMEM] * len(outs),
        out_shape=shapes,
        compiler_params=params(8),
    )(*operands)


def output_kernel(own, sqv_ref, p_ref, g_ref, *rest):
    out_ref, buf, sems = rest[-3:]
    core = lax.axis_index("core")
    half = core if own else 1 - core
    heads = p_ref.shape[0]
    parts, _, width = buf.shape
    per = 2 * heads // CHUNKS
    stores = []
    for h in range(heads):
        part, j = h // (heads // parts), h % (heads // parts)
        start = h // per * 3 * per * DH
        scores_qa = sqv_ref[0, :, start + 2 * (h % per) * DH : start + 2 * (h % per + 1) * DH]
        v = sqv_ref[0, :, head_cols(h % per, start + 2 * per * DH)]
        o = jnp.dot(
            scores_qa, jnp.concatenate([v, p_ref[h]], axis=0), preferred_element_type=f32
        )
        mean = jnp.mean(o * o, axis=-1, keepdims=True)
        normed = (o * lax.rsqrt(mean + EPSILON)).astype(bf16)
        gain = g_ref[:, pl.ds(pl.multiple_of(half * heads * DH + h * DH, DH), DH)]
        buf[part, :, head_cols(j)] = (normed.astype(f32) * gain).astype(bf16)
        if (h + 1) * DH == (part + 1) * width:
            cols = pl.ds(pl.multiple_of((half * parts + part) * width, width), width)
            store = pltpu.make_async_copy(buf.at[part], out_ref.at[0, :, cols], sems.at[part])
            store.start()
            stores.append(store)
    for store in stores:
        store.wait()


def half_outputs(sqv, prefix, gain, own, before=None):
    _, rows, width = sqv.shape
    width = width // 3
    in_specs, operands = [VMEM, VMEM, VMEM], [sqv, prefix, gain]
    if before is not None:
        in_specs.append(HBM)
        operands.append(before)
    return pl.pallas_call(
        functools.partial(output_kernel, own),
        in_specs=in_specs,
        out_specs=HBM,
        out_shape=jax.ShapeDtypeStruct((1, rows, 2 * width), bf16),
        scratch_shapes=[pltpu.VMEM((PARTS, rows, width // PARTS), bf16), DMA((PARTS,))],
        input_output_aliases={} if before is None else {3: 0},
        compiler_params=params(8),
        cost_estimate=cost(4 * 10**9),
        name="outputs",
    )(*operands)


def attend(queries, key_rows, value_rows, head_gain):
    swap = ((0, 1), (1, 0))
    owners, planes = lax.axis_size(OWNERS), lax.axis_size("z8")

    given = half_states(key_rows, value_rows, False)
    partner = lax.ppermute(given, "core", swap)
    kept = half_states(key_rows, value_rows, True)
    half = kept.shape
    chip, first = on_chip(merge_kernel, [half, half], kept, partner)
    pieces = (owners, chip.size // (owners * DH), DH)
    mine = lax.all_to_all(chip.reshape(pieces), OWNERS, 0, 0, tiled=True)
    (total,) = on_chip(total_kernel, [mine.shape[1:]], mine)
    span = planes // 2
    parts = within(queries, key_rows, value_rows, 0, EARLY, [total])
    total, *parts = lax.optimization_barrier((total, *parts))

    def ahead(k, value, low, high):
        return lax.ppermute(value, "z8", [(i, i + k) for i in range(low, high - k)])

    earlier = [ahead(1, total, 0, 2)]
    (front,) = on_chip(sum_kernel, [total.shape], total, *earlier)
    earlier += [ahead(k, front, 1, span) for k in range(span - 2, 0, -1)]
    parts = within(queries, key_rows, value_rows, EARLY, span, parts)
    (front,) = on_chip(sum_kernel, [total.shape], total, *earlier)
    earlier += [ahead(k, front, span - 1, planes) for k in range(planes - span, 0, -1)]
    sqv_own, sqv_other = within(queries, key_rows, value_rows, span, planes, parts)
    (prefixes,) = on_chip(prefix_kernel, [mine.shape], mine, *earlier)
    before = lax.all_to_all(prefixes, OWNERS, 0, 0, tiled=True)
    before = before.reshape(half)
    passed, used = on_chip(hand_over_kernel, [half, half], before, first)
    arrived = lax.ppermute(passed, "core", swap)
    gain = head_gain[None, :]
    out = half_outputs(sqv_own, used, gain, True)
    return half_outputs(sqv_other, arrived, gain, False, out)


def solution(mesh):
    torus = Mesh(mesh.devices.reshape(4, 2, 8, 2, 4), ("y", "core", "z8", "z2", "x"))
    spec = P(("z8", "z2", "x"), ("y", "core"), None)
    return jax.shard_map(
        attend, mesh=torus, in_specs=(spec, spec, spec, P()), out_specs=spec, check_vma=False
    )
```
